256 devices in a mesh: state: 256 (over y, z, x, core).
Axes of the slice: x: 4, y: 4, z: 8, core: 2. Of those that a mesh axis runs over, the one named last changes fastest.
Arguments:
- transitions: float32 [4096, 16, 4096], P('state'), may hold values from 0 to 1, as said below
- costs: float32 [4096, 16, 128], P('state'), may hold values from 0 to 4
- valid_counts: int32 [4096], P('state'), may hold values from 1 to 16
- start_values: float32 [4096, 128], P('state'), may hold values from -12 to 12
- ref_state: int32 [1], replicated, may hold values from 0 to 4095
Outputs:
- relative_values: float32 [4096, 128], P('state')
- lower_bounds: float32 [4, 128], replicated
- upper_bounds: float32 [4, 128], replicated
The draws below stay inside these ranges and needn't reach their ends.
Inputs may be any that keep to these rules, and one draw needn't show every extreme that they name: Every entry is nonnegative and each row transitions[s, a, :] sums to one up to float32 rounding. Actions 0 to valid_counts[s] - 1 are allowed in state s.
All inputs are finite; a program needn't handle non-finite values.
Results may differ from the reference program's by a relative error of at most 0.00017.
Values sent between devices are 32-bit elements; how exact they have to be, the bound alone decides.
A program may use at most 64 MiB of HBM per device.

```python
import jax
import jax.numpy as jnp
from jax import lax

STATES = 4096
ACTIONS = 16
SCENARIOS = 128
ITERS = 4


def draw_transitions(key, part):
    sigma = 2.0
    raw = jnp.exp(sigma * jax.random.normal(key, (STATES, ACTIONS, STATES), jnp.float32))
    return raw / jnp.sum(raw, axis=2, keepdims=True)


def place_ends(values, stream_key, low, top_value):
    extent = values.shape
    index_at = [jax.random.randint(jax.random.fold_in(stream_key, axis), (), 0, extent[axis]) for axis in range(len(extent))]
    values = values.at[tuple(index_at)].set(low)
    longest = extent.index(max(extent))
    index_at[longest] = (index_at[longest] + 1) % extent[longest]
    return values.at[tuple(index_at)].set(top_value)


def level_of(stream_key, dims, cuts, low, largest):
    def one(position, blocks):
        steps = jax.random.uniform(jax.random.fold_in(jax.random.fold_in(stream_key, 6), position), (blocks,), jnp.float32, low / len(cuts), largest / len(cuts))
        return jnp.repeat(jnp.exp(steps), dims[position] // blocks).reshape((-1,) + (1,) * (len(dims) - position - 1))

    factor_of = one(*cuts[0])
    for cut in cuts[1:]:
        factor_of = factor_of * one(*cut)
    return factor_of


def normal_values(stream_key, dims, deviation, bound, shards=(), held_as=jnp.bfloat16):
    loudness = level_of(stream_key, dims, shards, -0.22, 0.18) if shards else 1.0
    values = jax.random.normal(stream_key, dims, jnp.float32) * deviation * loudness
    return jnp.minimum(jnp.maximum(values, -bound), bound).astype(held_as)


def setup_inputs(seed: int = 0) -> dict:
    streams_of = jax.random.split(jax.random.key(seed), 6)
    return {
        "transitions": draw_transitions(jax.random.fold_in(streams_of[5], 71), 0),
        "costs": jnp.clip(4.0 * jax.random.uniform(streams_of[1], (STATES, ACTIONS, SCENARIOS), jnp.float32) ** level_of(streams_of[1], (STATES, ACTIONS, SCENARIOS), ((0, 256),), -0.2, 0.2), 0.0, 4.0),
        "valid_counts": place_ends(jax.random.randint(streams_of[2], (STATES,), 1, ACTIONS + 1), jax.random.fold_in(streams_of[2], 1), 1, ACTIONS).astype(jnp.int32),
        "start_values": normal_values(streams_of[3], (STATES, SCENARIOS), 2.0, 12.0, ((0, 256),), jnp.float32),
        "ref_state": jax.random.randint(streams_of[4], (1,), 0, STATES).astype(jnp.int32),
    }


big_value = 1e30


def reference(transitions, costs, valid_counts, start_values, ref_state):
    flat_rows = transitions.reshape(STATES * ACTIONS, STATES)
    allowed = jnp.arange(ACTIONS, dtype=jnp.int32)[None, :] < valid_counts[:, None]
    relative = start_values
    lower_list = []
    upper_list = []
    for iteration in range(ITERS):
        expected = jnp.dot(flat_rows, relative, precision=lax.Precision.HIGHEST, preferred_element_type=jnp.float32)
        q_values = costs + expected.reshape(STATES, ACTIONS, SCENARIOS)
        q_values = jnp.where(allowed[:, :, None], q_values, jnp.float32(big_value))
        best_value = jnp.min(q_values, axis=1)
        increase = best_value - relative
        lower_list.append(jnp.min(increase, axis=0))
        upper_list.append(jnp.max(increase, axis=0))
        ref_row = lax.dynamic_slice_in_dim(best_value, ref_state[0].astype(jnp.int32), 1, 0)
        relative = best_value - ref_row
    return relative, jnp.stack(lower_list), jnp.stack(upper_list)
```

```python
import functools

import jax
import jax.numpy as jnp
from jax import lax
from jax.experimental import pallas as pl
from jax.experimental.pallas import tpu as pltpu
from jax.sharding import Mesh
from jax.sharding import PartitionSpec as P

ITERS = 4
AXES = ("y", "z", "x", "c")
BIG = 1e30


def kernel(
    dims,
    t_hbm, costs, counts, start, ref_state,
    out, lower, upper,
    stage, t_hi, t_lo, values, split, masked, red, red_z, red_a, red_b, red_c,
    load_sem, ssem_z, rsem_z, ssem_f, rsem_f, ssem_d, rsem_d, ssem_r, rsem_r,
):
    ny, nz, nx = dims
    n = ny
    states, scenarios = start.shape
    actions = costs.shape[0] // states
    rows, width = t_hi.shape
    y, z, x, c = (lax.axis_index(a) for a in AXES)

    def dev(yy, zz, xx, cc):
        return {"y": yy, "z": zz, "x": xx, "c": cc}

    def shift(k, second):
        along_x = c if not second else 1 - c
        return lax.rem(y + k * (1 - along_x), n), lax.rem(x + k * along_x, n)

    def both(ka, kb):
        ya, xa = shift(ka, False)
        yb, xb = shift(kb, True)
        return jnp.where(c == 0, ya, yb), jnp.where(c == 0, xb, xa)

    def remote(src, dst, ssem, rsem, to):
        return pltpu.make_async_remote_copy(
            src_ref=src, dst_ref=dst, send_sem=ssem, recv_sem=rsem,
            device_id=to, device_id_type=pl.DeviceIdType.MESH,
        )

    load = pltpu.make_async_copy(t_hbm, stage, load_sem)
    load.start()

    barrier = pltpu.get_barrier_semaphore()

    def greet(to):
        pl.semaphore_signal(barrier, inc=1, device_id=to, device_id_type=pl.DeviceIdType.MESH)

    def greet_z(d, _):
        greet(dev(y, lax.rem(z + d, nz), x, c))
        return 0

    lax.fori_loop(1, nz, greet_z, 0)

    def greet_plane(k, _):
        ya, xa = shift(k, False)
        greet(dev(ya, z, xa, c))
        yb, xb = shift(k, True)
        greet(dev(yb, z, xb, c))
        return 0

    lax.fori_loop(1, n, greet_plane, 0)
    greet(dev(y, z, x, 1 - c))

    values[0, y, z, x, c] = start[...]
    action = lax.broadcasted_iota(jnp.int32, (actions, scenarios), 0)
    for s in range(states):
        block = pl.ds(s * actions, actions)
        masked[block, :] = jnp.where(action < counts[s], costs[block, :], jnp.float32(BIG))

    pl.semaphore_wait(barrier, nz - 1 + 2 * (n - 1) + 1)

    def gather(t, p):
        own = values.at[t, y, z, x, c]

        def column(yy, xx):
            return values.at[t, yy, :, xx, c]

        def send_z(d, _):
            zz = lax.rem(z + d, nz)
            remote(own, own, ssem_z.at[d], rsem_z.at[p, z], dev(y, zz, x, c)).start()
            return 0

        lax.fori_loop(1, nz, send_z, 0)

        def wait_z(d, _):
            zz = lax.rem(z + d, nz)
            there = values.at[t, y, zz, x, c]
            remote(there, there, ssem_z.at[d], rsem_z.at[p, zz], dev(y, zz, x, c)).wait_recv()
            return 0

        lax.fori_loop(1, nz, wait_z, 0)

        def forward(k, yy, xx, second):
            def one(j, _):
                yt, xt = shift(j, second)
                slot = jnp.where(second, 1 + k, 0)
                remote(column(yy, xx), column(yy, xx), ssem_f.at[slot, j], rsem_f.at[p, yy, xx], dev(yt, z, xt, c)).start()
                return 0

            lax.fori_loop(1, n, one, 0)

        def across(yy, xx):
            remote(column(yy, xx), column(yy, xx), ssem_d.at[yy, xx], rsem_d.at[p, yy, xx], dev(y, z, x, 1 - c)).start()

        def arrived(yy, xx):
            remote(column(yy, xx), column(yy, xx), ssem_f.at[0, 0], rsem_f.at[p, yy, xx], dev(y, z, x, 1 - c)).wait_recv()

        forward(0, y, x, False)
        forward(0, y, x, True)
        across(y, x)

        def first(k, _):
            yy, xx = shift(k, False)
            arrived(yy, xx)
            forward(k, yy, xx, True)
            across(yy, xx)
            return 0

        lax.fori_loop(1, n, first, 0)

        def second(i, _):
            j = 1 + i // n
            yy, xx = both(i % n, j)
            arrived(yy, xx)
            across(yy, xx)
            return 0

        lax.fori_loop(0, (n - 1) * n, second, 0)

        def partner(i, _):
            yy, xx = i // n, i % n
            there = values.at[t, yy, :, xx, 1 - c]
            remote(there, there, ssem_d.at[yy, xx], rsem_d.at[p, yy, xx], dev(y, z, x, 1 - c)).wait_recv()
            remote(column(yy, xx), column(yy, xx), ssem_d.at[yy, xx], rsem_d.at[p, yy, xx], dev(y, z, x, 1 - c)).wait_send()
            return 0

        lax.fori_loop(0, n * n, partner, 0)

        def sent_z(d, _):
            remote(own, own, ssem_z.at[d], rsem_z.at[p, z], dev(y, z, x, 1 - c)).wait_send()
            return 0

        lax.fori_loop(1, nz, sent_z, 0)

        def sent_f(i, _):
            remote(column(y, x), column(y, x), ssem_f.at[i // (n - 1), 1 + i % (n - 1)], rsem_f.at[p, y, x], dev(y, z, x, 1 - c)).wait_send()
            return 0

        lax.fori_loop(0, (n + 1) * (n - 1), sent_f, 0)

    def split_rows():
        load.wait()

        def one(i, _):
            block = pl.ds(pl.multiple_of(i * 16, 16), 16)
            whole = stage[block, :]
            high = whole.astype(jnp.bfloat16)
            t_hi[block, :] = high
            t_lo[block, :] = (whole - high.astype(jnp.float32)).astype(jnp.bfloat16)
            return 0

        lax.fori_loop(0, rows // 16, one, 0)

    split_rows()
    per = nx * 2 * states

    def iterate(t, _):
        gather(t, lax.rem(t, 2))

        def halves(i, _):
            block = values[t, i // nz, i % nz].reshape(per, scenarios)
            high = block.astype(jnp.bfloat16)
            at = pl.ds(pl.multiple_of(i * per, per), per)
            split[at, :scenarios] = high
            split[at, scenarios:] = (block - high.astype(jnp.float32)).astype(jnp.bfloat16)
            return 0

        lax.fori_loop(0, ny * nz, halves, 0)
        right = split[...]
        total = jnp.dot(t_hi[...], right, preferred_element_type=jnp.float32)
        total += jnp.dot(t_lo[...], right, preferred_element_type=jnp.float32)
        q_values = masked[...] + (total[:, :scenarios] + total[:, scenarios:])
        best = jnp.min(q_values.reshape(states, actions, scenarios), axis=1)
        increase = best - values[t, y, z, x, c]
        red[pl.ds(t, 1), :] = jnp.max(increase, axis=0, keepdims=True)
        red[pl.ds(ITERS + t, 1), :] = jnp.max(-increase, axis=0, keepdims=True)

        @pl.when(t < ITERS - 1)
        def _():
            values[t + 1, y, z, x, c] = best

        @pl.when(t == ITERS - 1)
        def _():
            out[...] = best
        return 0

    lax.fori_loop(0, ITERS, iterate, 0)

    me = ((y * nz + z) * nx + x) * 2 + c
    row = me * states + lax.broadcasted_iota(jnp.int32, (states, scenarios), 0)
    ref_row = jnp.max(jnp.where(row == ref_state[0], out[...], jnp.float32(-BIG)), axis=0, keepdims=True)
    red[2 * ITERS:, :] = jnp.broadcast_to(ref_row, (8, scenarios))

    def exchange(buffer, count, index, to, sem):
        def go(d, _):
            remote(red, buffer.at[index(0)], ssem_r.at[sem + d], rsem_r.at[sem + index(0)], to(d)).start()
            return 0

        lax.fori_loop(1, count, go, 0)

        def done(d, _):
            remote(red, buffer.at[index(d)], ssem_r.at[sem + d], rsem_r.at[sem + index(d)], to(d)).wait()
            return 0

        lax.fori_loop(1, count, done, 0)
        best = red[...]
        for d in range(1, count):
            best = jnp.maximum(best, buffer[index(d)])
        red[...] = best

    exchange(red_z, nz, lambda d: lax.rem(z + d, nz), lambda d: dev(y, lax.rem(z + d, nz), x, c), 0)

    def place(second):
        def index(d):
            yy, xx = shift(d, second)
            along_x = c if not second else 1 - c
            return jnp.where(along_x == 1, xx, yy)

        def to(d):
            yy, xx = shift(d, second)
            return dev(yy, z, xx, c)

        return index, to

    exchange(red_a, n, *place(False), nz)
    exchange(red_b, n, *place(True), nz + n)
    exchange(red_c, 2, lambda d: lax.rem(c + d, 2), lambda d: dev(y, z, x, 1 - c), nz + 2 * n)

    upper[...] = red[:ITERS, :]
    lower[...] = -red[ITERS:2 * ITERS, :]
    out[...] = out[...] - red[2 * ITERS:2 * ITERS + 1, :]


def local(dims, transitions, costs, counts, start, ref_state):
    states, actions, width = transitions.shape
    scenarios = start.shape[1]
    rows = states * actions
    ny, nz, nx = dims
    n = ny
    block = (states, scenarios)
    dma = pltpu.SemaphoreType.DMA
    vmem = pl.BlockSpec(memory_space=pltpu.VMEM)
    smem = pl.BlockSpec(memory_space=pltpu.SMEM)
    return pl.pallas_call(
        functools.partial(kernel, dims),
        out_shape=(
            jax.ShapeDtypeStruct(block, jnp.float32),
            jax.ShapeDtypeStruct((ITERS, scenarios), jnp.float32),
            jax.ShapeDtypeStruct((ITERS, scenarios), jnp.float32),
        ),
        in_specs=[pl.BlockSpec(memory_space=pl.ANY), vmem, smem, vmem, smem],
        out_specs=(vmem, vmem, vmem),
        scratch_shapes=[
            pltpu.VMEM((rows, width), jnp.float32),
            pltpu.VMEM((rows, width), jnp.bfloat16),
            pltpu.VMEM((rows, width), jnp.bfloat16),
            pltpu.VMEM((ITERS, ny, nz, nx, 2) + block, jnp.float32),
            pltpu.VMEM((width, 2 * scenarios), jnp.bfloat16),
            pltpu.VMEM((rows, scenarios), jnp.float32),
            pltpu.VMEM(block, jnp.float32),
            pltpu.VMEM((nz,) + block, jnp.float32),
            pltpu.VMEM((n,) + block, jnp.float32),
            pltpu.VMEM((n,) + block, jnp.float32),
            pltpu.VMEM((2,) + block, jnp.float32),
            dma,
            dma((nz,)),
            dma((2, nz)),
            dma((n + 1, n)),
            dma((2, n, n)),
            dma((n, n)),
            dma((2, n, n)),
            dma((nz + 2 * n + 2,)),
            dma((nz + 2 * n + 2,)),
        ],
        compiler_params=pltpu.CompilerParams(collective_id=0, has_side_effects=True),
    )(transitions.reshape(rows, width), costs.reshape(rows, scenarios), counts, start, ref_state)


def solution(mesh):
    dims = (4, 8, 4)
    split = Mesh(mesh.devices.reshape(dims + (2,)), AXES)
    return jax.shard_map(
        functools.partial(local, dims),
        mesh=split,
        in_specs=(P(AXES, None, None), P(AXES, None, None), P(AXES), P(AXES, None), P()),
        out_specs=(P(AXES, None), P(), P()),
        check_vma=False,
    )
```
